128 devices in a mesh: mem: 16 (over y, x), pix: 8 (over z, core).
Axes of the slice: x: 4, y: 4, z: 4, core: 2. Of those that a mesh axis runs over, the one named last changes fastest.
Arguments:
- prior_motion: bfloat16 [64, 16, 262144], P('mem', None, 'pix'), may hold values from -6 to 6
- measured_motion: float32 [1200], replicated, may hold values from -1.6 to 1.6
- measurement_noise_stddev: float32 [1200], replicated, may hold values from 0.05 to 0.5
- gaussian_jitter: float32 [2, 1200, 64], replicated, may hold values from -6 to 6
- scene_couples: int32 [2, 1200], replicated, may hold values from 0 to 15, as said below
- targeted_tile_number: int32 [1200], replicated, may hold values from 0 to 4095
Outputs:
- analysis: bfloat16 [64, 16, 262144], P('mem', None, 'pix')
The draws below stay inside these ranges and needn't reach their ends.
Inputs may be any that keep to these rules, and one draw needn't show every extreme that they name: scene_couples[0, k] < scene_couples[1, k]: row 0 holds the earlier acquisition, row 1 the later.
All inputs are finite; a program needn't handle non-finite values.
Results may differ from the reference program's by a relative error of at most 0.011.
Values may be sent and summed in bfloat16 or wider, within the bound.
A program may use at most 128 MiB of HBM per device.

```python
import math
import jax
import jax.numpy as jnp
from jax import lax

REALIZATION_NUM = 64
SCENE_TIMES = 16
NOBS = 1200
BLK = 64
PASS_COUNT = 2
RASTER_CELLS = 262144
NBLK = 4096
N_MEM = 16
N_PIX = 8


def draw_scene_couples(key, part):
    key_first = jax.random.fold_in(key, 11)
    key_gap = jax.random.fold_in(key, 12)
    earlier = jax.random.randint(key_first, (NOBS,), 0, SCENE_TIMES - 1)
    offset = jax.random.randint(key_gap, (NOBS,), 0, SCENE_TIMES - 1)
    later = earlier + 1 + offset % (SCENE_TIMES - 1 - earlier)
    return jnp.stack([earlier, later]).astype(jnp.int32)


def plant(entries, rng, least, largest):
    extent = entries.shape
    index_at = [jax.random.randint(jax.random.fold_in(rng, axis), (), 0, extent[axis]) for axis in range(len(extent))]
    entries = entries.at[tuple(index_at)].set(least)
    longest = extent.index(max(extent))
    index_at[longest] = (index_at[longest] + 1) % extent[longest]
    return entries.at[tuple(index_at)].set(largest)


def level_of(key, extent, split, low, top_value):
    factor_of, own = 1.0, jax.random.fold_in(key, 6)
    for position, blocks in split:
        draws = jnp.exp(jax.random.uniform(jax.random.fold_in(own, position), (blocks,), jnp.float32, low / len(split), top_value / len(split)))
        factor_of = factor_of * jnp.repeat(draws, extent[position] // blocks).reshape([-1 if axis == position else 1 for axis in range(len(extent))])
    return factor_of


def noise(key, shape, width, most, split=(), kind=jnp.bfloat16):
    entries = jax.random.normal(key, shape, jnp.float32) * width
    if len(split) > 0:
        entries = level_of(key, shape, split, -0.22, 0.18) * entries
    return jnp.clip(entries, min=-most, max=most).astype(kind)


def setup_inputs(seed: int = 0) -> dict:
    arg_keys = jax.random.split(jax.random.key(seed), 7)
    prior_motion = noise(arg_keys[0], (REALIZATION_NUM, SCENE_TIMES, RASTER_CELLS), 1.0, 6.0, ((0, 16), (2, 8)))
    measured_motion = noise(arg_keys[1], (NOBS,), 0.2, 1.6, (), jnp.float32)
    measurement_noise_stddev = jnp.clip(jnp.exp(jax.random.uniform(arg_keys[2], (NOBS,), jnp.float32, math.log(0.05), math.log(0.5))), 0.05, 0.5)
    gaussian_jitter = noise(arg_keys[3], (PASS_COUNT, NOBS, REALIZATION_NUM), 1.0, 6.0, (), jnp.float32)
    scene_couples = draw_scene_couples(jax.random.fold_in(arg_keys[6], 71), 0)
    targeted_tile_number = plant(jax.random.randint(arg_keys[5], (NOBS,), 0, NBLK), jax.random.fold_in(arg_keys[5], 1), 0, NBLK - 1).astype(jnp.int32)
    return {"prior_motion": prior_motion, "measured_motion": measured_motion, "measurement_noise_stddev": measurement_noise_stddev, "gaussian_jitter": gaussian_jitter, "scene_couples": scene_couples, "targeted_tile_number": targeted_tile_number}


def update_tile(tile_state, mixing):
    realization_vectors = tile_state.shape[0]
    average = lax.optimization_barrier(jnp.sum(tile_state, axis=0, dtype=jnp.float32)) / realization_vectors
    anomaly = (tile_state.astype(jnp.float32) - average).astype(jnp.bfloat16)
    change = jnp.dot(mixing.T.astype(jnp.float32), anomaly.reshape(realization_vectors, -1).astype(jnp.float32), preferred_element_type=jnp.float32)
    return (tile_state.astype(jnp.float32) + change.reshape(tile_state.shape)).astype(jnp.bfloat16)

def reference(prior_motion, measured_motion, measurement_noise_stddev, gaussian_jitter, scene_couples, targeted_tile_number):
    realization_vectors = prior_motion.shape[0]
    spread_factor = float(PASS_COUNT)
    member_anomaly = jnp.sqrt(jnp.float32(spread_factor)) * measurement_noise_stddev
    ground_motion_vector = prior_motion
    for iteration in range(PASS_COUNT):
        sums = lax.optimization_barrier(jnp.sum(ground_motion_vector.reshape(realization_vectors, SCENE_TIMES, NBLK, BLK), axis=3, dtype=jnp.float32))
        predicted = ((sums[:, scene_couples[1], targeted_tile_number] - sums[:, scene_couples[0], targeted_tile_number]) / BLK).T
        centred = predicted - lax.optimization_barrier(jnp.mean(predicted, axis=1, keepdims=True))
        scaled = centred / (member_anomaly[:, None] * math.sqrt(realization_vectors - 1))
        misfit = (measured_motion[:, None] + member_anomaly[:, None] * gaussian_jitter[iteration] - predicted) / member_anomaly[:, None]
        gram = jnp.dot(scaled.T.astype(jnp.float32), scaled.astype(jnp.float32), precision=lax.Precision.HIGHEST, preferred_element_type=jnp.float32)
        cross = jnp.dot(scaled.T.astype(jnp.float32), misfit.astype(jnp.float32), precision=lax.Precision.HIGHEST, preferred_element_type=jnp.float32)
        factor = jnp.linalg.cholesky(jnp.eye(realization_vectors, dtype=jnp.float32) + gram)
        mixing = (jax.scipy.linalg.cho_solve((factor, True), cross) / math.sqrt(realization_vectors - 1)).astype(jnp.bfloat16)
        tiles = jnp.moveaxis(ground_motion_vector.reshape(realization_vectors, SCENE_TIMES, N_PIX * N_MEM, -1), 2, 0)

        def one_tile(tile_state):
            return update_tile(tile_state, mixing)
        fresh = lax.map(one_tile, tiles)
        ground_motion_vector = jnp.moveaxis(fresh, 0, 2).reshape(ground_motion_vector.shape)
    return ground_motion_vector
```

```python
import functools
import math

import jax
import jax.numpy as jnp
from jax import lax
from jax.experimental import pallas as pl
from jax.experimental.pallas import tpu as pltpu
from jax.sharding import PartitionSpec as P

MESH = pl.DeviceIdType.MESH
HIGHEST = lax.Precision.HIGHEST
BLK = 64
PASS_COUNT = 2
MEMBERS = 64
TIMES = 16
NOBS = 1200
OBS = 1280
HALF = OBS // 2
OWN = 4
CELLS = 32768
PART = 2048
BLOCKS = CELLS // BLK
NPIX = 8
STEPS = 4
COLS = PART // STEPS
GROUP = 4
ROOT = math.sqrt(MEMBERS - 1)

ORDER = (
    (0, 1), (1, 0), (0, 3), (3, 0), (1, 1), (3, 3), (1, 3), (3, 1),
    (2, 2), (0, 2), (2, 0), (1, 2), (2, 1), (3, 2), (2, 3),
)
EARLY = 15


def iota(shape, axis):
    return lax.broadcasted_iota(jnp.int32, shape, axis)


def f32_dot(a, b, dims=((1,), (0,))):
    return lax.dot_general(a, b, (dims, ((), ())), precision=HIGHEST, preferred_element_type=jnp.float32)


def bf16_dot(a, b):
    return jnp.dot(a, b, preferred_element_type=jnp.float32)


def solve(system):
    row_at = iota(system.shape, 0)
    for start in range(0, MEMBERS, GROUP):
        columns = [jnp.broadcast_to(system[:, start + j : start + j + 1], system.shape) for j in range(GROUP)]
        for j in range(GROUP):
            k = start + j
            here = row_at == k
            inverse = 1.0 / columns[j][k : k + 1, :]
            pivot_row = system[k : k + 1, :] * inverse
            for later in range(j + 1, GROUP):
                share = columns[later][k : k + 1, :] * inverse
                columns[later] = jnp.where(here, share, columns[later] - columns[j] * share)
            system = jnp.where(here, pivot_row, system - columns[j] * pivot_row)
    return system[:, MEMBERS:]


def kernel(
    prior, obs, jitter, out,
    own, received, result, spread, noise, part_pred, pix_pred, whole_pred, mem_pred, predicted,
    load_sem, noise_sem, self_sem, put_sem,
    send_sem, recv_sem, pix_send, pix_recv, mem_send, mem_recv, back_send, back_recv,
):
    mem = lax.axis_index("mem")
    pix = lax.axis_index("pix")
    y = mem // 4
    x = mem % 4
    partners = [(((y + dy) % 4) * 4 + (x + dx) % 4) for dy, dx in ORDER]
    lines = [(pix + d) % NPIX for d in range(1, NPIX)]

    barrier = pltpu.get_barrier_semaphore()
    for p in partners:
        pl.semaphore_signal(barrier, 1, device_id=(p, pix), device_id_type=MESH)
    for p in lines:
        pl.semaphore_signal(barrier, 1, device_id=(mem, p), device_id_type=MESH)

    load = pltpu.make_async_copy(prior, own, load_sem)
    load.start()
    mine = pltpu.make_async_copy(
        prior.at[:, :, pl.ds(pl.multiple_of(mem * PART, PART), PART)],
        received.at[pl.ds(OWN * mem, OWN)],
        self_sem,
    )
    mine.start()
    noises = [pltpu.make_async_copy(jitter.at[i], noise.at[i, pl.ds(0, NOBS)], noise_sem.at[i]) for i in range(PASS_COUNT)]
    for copy in noises:
        copy.start()
    for i in range(PASS_COUNT):
        noise[i, NOBS:, :] = jnp.zeros((OBS - NOBS, MEMBERS), jnp.float32)

    pl.semaphore_wait(barrier, len(partners) + len(lines))

    def outgoing(s, i):
        p = partners[i]
        return pltpu.make_async_remote_copy(
            prior.at[pl.ds(s, 1), :, pl.ds(pl.multiple_of(p * PART, PART), PART)],
            received.at[pl.ds(OWN * mem + s, 1)],
            send_sem.at[s, i],
            recv_sem.at[s, i],
            device_id=(p, pix),
            device_id_type=MESH,
        )

    outgoings = [outgoing(s, i) for s in range(OWN) for i in range(len(ORDER))]
    for copy in outgoings[:EARLY]:
        copy.start()

    load.wait()
    depth = 1024

    def add_blocks(step, total):
        ones = jnp.where(iota((depth, 128), 1) - (iota((depth, 128), 0) >> 6) == step * (depth // BLK), 1.0, 0.0)
        rows = [
            own[:, :, pl.ds(pl.multiple_of(c * 8192 + step * depth, depth), depth)].reshape(OWN * TIMES, depth)
            for c in range(4)
        ]
        return total + bf16_dot(jnp.concatenate(rows, axis=0), ones.astype(jnp.bfloat16))

    sums = lax.fori_loop(0, 8192 // depth, add_blocks, jnp.zeros((4 * OWN * TIMES, 128), jnp.float32))
    sums = jnp.concatenate([sums[c * 64 : (c + 1) * 64] for c in range(4)], axis=1)
    high = sums.astype(jnp.bfloat16)
    rest = sums - high.astype(jnp.float32)
    middle = rest.astype(jnp.bfloat16)
    low = (rest - middle.astype(jnp.float32)).astype(jnp.bfloat16)
    parts = jnp.concatenate([high, middle, low], axis=0)

    for h in range(2):
        lanes = slice(h * HALF, (h + 1) * HALF)
        block = obs[2:3, lanes].astype(jnp.int32) - pix * BLOCKS
        pick = jnp.where(iota((BLOCKS, HALF), 0) == block, 1.0, 0.0).astype(jnp.bfloat16)
        seen = bf16_dot(parts, pick)
        seen = seen[0:64] + seen[64:128] + seen[128:192]
        scene = iota((TIMES, HALF), 0)
        pair = jnp.where(scene == obs[4:5, lanes].astype(jnp.int32), 1.0, 0.0) - jnp.where(
            scene == obs[3:4, lanes].astype(jnp.int32), 1.0, 0.0
        )
        part_pred[h * OWN : (h + 1) * OWN, :] = (
            jnp.sum(seen.reshape(OWN, TIMES, HALF) * pair[None], axis=1) * (1.0 / BLK)
        )

    line_copies = [
        pltpu.make_async_remote_copy(
            part_pred, pix_pred.at[pix], pix_send.at[d], pix_recv.at[d], device_id=(mem, p), device_id_type=MESH
        )
        for d, p in enumerate(lines)
    ]
    for copy in line_copies:
        copy.start()
    for copy in line_copies:
        copy.wait()
    whole = part_pred[...]
    for p in lines:
        whole = whole + pix_pred[p]
    whole_pred[...] = whole
    mem_pred[mem] = whole

    plane_copies = [
        pltpu.make_async_remote_copy(
            whole_pred, mem_pred.at[mem], mem_send.at[d], mem_recv.at[d], device_id=(p, pix), device_id_type=MESH
        )
        for d, p in enumerate(partners)
    ]
    for copy in plane_copies:
        copy.start()
    for copy in outgoings[EARLY:]:
        copy.start()
    for copy in noises:
        copy.wait()
    for copy in plane_copies:
        copy.wait()

    for s in range(16):
        for h in range(2):
            predicted[OWN * s : OWN * (s + 1), h * HALF : (h + 1) * HALF] = mem_pred[s, h * OWN : (h + 1) * OWN, :]

    error = obs[1:2, :] * math.sqrt(float(PASS_COUNT))
    pred = predicted[...]
    mean = jnp.sum(pred, axis=0, keepdims=True) * (1.0 / MEMBERS)
    scaled = (pred - mean) / (error * ROOT)
    offset = jnp.sum(scaled * ((obs[0:1, :] - mean) / error), axis=1, keepdims=True)
    gram = f32_dot(scaled, scaled, ((1,), (1,)))
    cross = [f32_dot(scaled, noise[i]) + offset for i in range(PASS_COUNT)]
    eye = jnp.where(iota((MEMBERS, MEMBERS), 0) == iota((MEMBERS, MEMBERS), 1), 1.0, 0.0)

    def rounded(solved):
        return (solved * (1.0 / ROOT)).astype(jnp.bfloat16).astype(jnp.float32)

    first = rounded(solve(jnp.concatenate([eye + gram, cross[0] - ROOT * gram], axis=1)))
    moved = f32_dot(gram, first)
    change = eye + first - jnp.mean(first, axis=1, keepdims=True)
    both = gram + moved
    right = jnp.concatenate([both - jnp.mean(moved, axis=1, keepdims=True), cross[1] - ROOT * both], axis=1)
    system = f32_dot(change.T, right)
    second = rounded(solve(system + jnp.concatenate([eye, jnp.zeros_like(eye)], axis=1)))
    one = first - jnp.mean(first, axis=0, keepdims=True)
    two = second - jnp.mean(second, axis=0, keepdims=True)
    total = one + two + f32_dot(one, two)

    widen = jnp.where(iota((MEMBERS, MEMBERS * TIMES), 1) >> 4 == iota((MEMBERS, MEMBERS * TIMES), 0), 1.0, 0.0)
    wide = bf16_dot(total.T.astype(jnp.bfloat16), widen.astype(jnp.bfloat16))
    same = (iota((TIMES, MEMBERS * TIMES), 1) & (TIMES - 1)) == iota((TIMES, MEMBERS * TIMES), 0)
    for j in range(MEMBERS):
        spread[j * TIMES : (j + 1) * TIMES, :] = jnp.where(same, wide[j : j + 1, :], 0.0).astype(jnp.bfloat16)

    mine.wait()
    for copy in outgoings:
        copy.wait()

    def incoming(step, i):
        p = partners[i]
        return pltpu.make_async_remote_copy(
            result.at[pl.ds(OWN * p, OWN), :, pl.ds(pl.multiple_of(step * COLS, COLS), COLS)],
            out.at[:, :, pl.ds(pl.multiple_of(mem * PART + step * COLS, COLS), COLS)],
            back_send.at[step, i],
            back_recv.at[step, i],
            device_id=(p, pix),
            device_id_type=MESH,
        )

    def keep(step):
        return pltpu.make_async_copy(
            result.at[pl.ds(OWN * mem, OWN), :, pl.ds(pl.multiple_of(step * COLS, COLS), COLS)],
            out.at[:, :, pl.ds(pl.multiple_of(mem * PART + step * COLS, COLS), COLS)],
            put_sem.at[step],
        )

    def advance(step, carry):
        lanes = pl.ds(pl.multiple_of(step * COLS, COLS), COLS)
        state = received[:, :, lanes].reshape(MEMBERS * TIMES, COLS)
        for r in range(4):
            members = slice(r * 16, (r + 1) * 16)
            rows = slice(r * 256, (r + 1) * 256)
            moved = bf16_dot(spread[rows, :], state)
            fresh = received[members, :, lanes].reshape(256, COLS).astype(jnp.float32) + moved
            result[members, :, lanes] = fresh.astype(jnp.bfloat16).reshape(16, TIMES, COLS)
        for i in range(len(ORDER)):
            incoming(step, i).start()
        keep(step).start()
        return carry

    lax.fori_loop(0, STEPS, advance, 0)

    def finish(step, carry):
        for i in range(len(ORDER)):
            incoming(step, i).wait()
        keep(step).wait()
        return carry

    lax.fori_loop(0, STEPS, finish, 0)


def body(prior_motion, measured_motion, measurement_noise_stddev, gaussian_jitter, scene_couples, targeted_tile_number):
    def row(values, fill):
        return jnp.pad(values.astype(jnp.float32), (0, OBS - NOBS), constant_values=fill)[None]

    obs = jnp.concatenate(
        [
            row(measured_motion, 0.0),
            row(measurement_noise_stddev, 1.0),
            row(targeted_tile_number, -1.0),
            row(scene_couples[0], 0.0),
            row(scene_couples[1], 0.0),
            jnp.zeros((3, OBS), jnp.float32),
        ],
        axis=0,
    )
    anywhere = pl.BlockSpec(memory_space=pl.ANY)
    dma = pltpu.SemaphoreType.DMA
    n = len(ORDER)
    return pl.pallas_call(
        kernel,
        out_shape=jax.ShapeDtypeStruct(prior_motion.shape, jnp.bfloat16),
        in_specs=[anywhere, pl.BlockSpec(memory_space=pltpu.VMEM), anywhere],
        out_specs=anywhere,
        scratch_shapes=[
            pltpu.VMEM((OWN, TIMES, CELLS), jnp.bfloat16),
            pltpu.VMEM((MEMBERS, TIMES, PART), jnp.bfloat16),
            pltpu.VMEM((MEMBERS, TIMES, PART), jnp.bfloat16),
            pltpu.VMEM((MEMBERS * TIMES, MEMBERS * TIMES), jnp.bfloat16),
            pltpu.VMEM((PASS_COUNT, OBS, MEMBERS), jnp.float32),
            pltpu.VMEM((2 * OWN, HALF), jnp.float32),
            pltpu.VMEM((NPIX, 2 * OWN, HALF), jnp.float32),
            pltpu.VMEM((2 * OWN, HALF), jnp.float32),
            pltpu.VMEM((16, 2 * OWN, HALF), jnp.float32),
            pltpu.VMEM((MEMBERS, OBS), jnp.float32),
            dma, dma((PASS_COUNT,)), dma, dma((STEPS,)),
            dma((OWN, n)), dma((OWN, n)),
            dma((NPIX - 1,)), dma((NPIX - 1,)),
            dma((n,)), dma((n,)),
            dma((STEPS, n)), dma((STEPS, n)),
        ],
        compiler_params=pltpu.CompilerParams(collective_id=0, has_side_effects=True, vmem_limit_bytes=60 << 20),
        name="smoother",
    )(prior_motion, obs, gaussian_jitter)


def solution(mesh):
    return jax.shard_map(
        body,
        mesh=mesh,
        in_specs=(P("mem", None, "pix"), P(), P(), P(), P(), P()),
        out_specs=P("mem", None, "pix"),
        check_vma=False,
    )
```

```python
import functools
import math

import jax
import jax.numpy as jnp
from jax import lax
from jax.experimental import pallas as pl
from jax.experimental.pallas import tpu as pltpu
from jax.sharding import PartitionSpec as P

MESH = pl.DeviceIdType.MESH
HIGHEST = lax.Precision.HIGHEST
BLK = 64
PASS_COUNT = 2
MEMBERS = 64
TIMES = 16
NOBS = 1200
OBS = 1280
HALF = OBS // 2
OWN = 4
CELLS = 32768
PART = 2048
BLOCKS = CELLS // BLK
NPIX = 8
STEPS = 4
COLS = PART // STEPS
GROUP = 4
ROOT = math.sqrt(MEMBERS - 1)

ORDER = (
    (0, 1), (1, 0), (0, 3), (3, 0), (1, 1), (3, 3), (1, 3), (3, 1),
    (2, 2), (0, 2), (2, 0), (1, 2), (2, 1), (3, 2), (2, 3),
)
EARLY = 30


def iota(shape, axis):
    return lax.broadcasted_iota(jnp.int32, shape, axis)


def f32_dot(a, b, dims=((1,), (0,))):
    return lax.dot_general(a, b, (dims, ((), ())), precision=HIGHEST, preferred_element_type=jnp.float32)


def bf16_dot(a, b):
    return jnp.dot(a, b, preferred_element_type=jnp.float32)


def solve(system):
    row_at = iota(system.shape, 0)
    for start in range(0, MEMBERS, GROUP):
        columns = [jnp.broadcast_to(system[:, start + j : start + j + 1], system.shape) for j in range(GROUP)]
        for j in range(GROUP):
            k = start + j
            here = row_at == k
            inverse = 1.0 / columns[j][k : k + 1, :]
            pivot_row = system[k : k + 1, :] * inverse
            for later in range(j + 1, GROUP):
                share = columns[later][k : k + 1, :] * inverse
                columns[later] = jnp.where(here, share, columns[later] - columns[j] * share)
            system = jnp.where(here, pivot_row, system - columns[j] * pivot_row)
    return system[:, MEMBERS:]


def kernel(
    prior, measured, stddev, jitter, couples, tiles, out,
    own, received, result, spread, keeps, noise, pairs, table,
    part_pred, pix_pred, whole_pred, mem_pred, predicted,
    load_sem, small_sem, self_sem,
    send_sem, recv_sem, pix_send, pix_recv, mem_send, mem_recv, back_send, back_recv,
):
    mem = lax.axis_index("mem")
    pix = lax.axis_index("pix")
    y = mem // 4
    x = mem % 4
    partners = [(((y + dy) % 4) * 4 + (x + dx) % 4) for dy, dx in ORDER]
    lines = [(pix + d) % NPIX for d in range(1, NPIX)]

    barrier = pltpu.get_barrier_semaphore()
    for p in partners:
        pl.semaphore_signal(barrier, 1, device_id=(p, pix), device_id_type=MESH)
    for p in lines:
        pl.semaphore_signal(barrier, 1, device_id=(mem, p), device_id_type=MESH)

    load = pltpu.make_async_copy(prior, own, load_sem)
    load.start()
    mine = pltpu.make_async_copy(
        prior.at[:, :, pl.ds(pl.multiple_of(mem * PART, PART), PART)],
        received.at[pl.ds(OWN * mem, OWN)],
        self_sem,
    )
    mine.start()
    smalls = [
        pltpu.make_async_copy(src, dst, small_sem.at[i])
        for i, (src, dst) in enumerate(
            ((couples, pairs), (jitter, noise))
        )
    ]
    for copy in smalls:
        copy.start()
    table[...] = jnp.full(table.shape, -1, jnp.int32)

    pl.semaphore_wait(barrier, len(partners) + len(lines))

    def columns(start, step):
        return pl.ds(pl.multiple_of(start * PART + step * COLS, COLS), COLS)

    def outgoing(s, i):
        p = partners[i]
        return pltpu.make_async_remote_copy(
            prior.at[:, :, columns(p, s)],
            received.at[pl.ds(OWN * mem, OWN), :, pl.ds(s * COLS, COLS)],
            send_sem.at[s, i],
            recv_sem.at[s, i],
            device_id=(p, pix),
            device_id_type=MESH,
        )

    outgoings = [outgoing(s, i) for s in range(STEPS) for i in range(len(ORDER))]
    for copy in outgoings[:EARLY]:
        copy.start()

    load.wait()
    depth = 1024

    def add_blocks(step, total):
        ones = jnp.where(iota((depth, 128), 1) - (iota((depth, 128), 0) >> 6) == step * (depth // BLK), 1.0, 0.0)
        rows = [
            own[:, :, pl.ds(pl.multiple_of(c * 8192 + step * depth, depth), depth)].reshape(OWN * TIMES, depth)
            for c in range(4)
        ]
        return total + bf16_dot(jnp.concatenate(rows, axis=0), ones.astype(jnp.bfloat16))

    sums = lax.fori_loop(0, 8192 // depth, add_blocks, jnp.zeros((4 * OWN * TIMES, 128), jnp.float32))
    sums = jnp.concatenate([sums[c * 64 : (c + 1) * 64] for c in range(4)], axis=1)
    high = sums.astype(jnp.bfloat16)
    rest = sums - high.astype(jnp.float32)
    middle = rest.astype(jnp.bfloat16)
    low = (rest - middle.astype(jnp.float32)).astype(jnp.bfloat16)
    parts = jnp.concatenate([high, middle, low], axis=0)

    smalls[0].wait()
    table[0:2, 0:NOBS] = pairs[...]
    table[2:3, 0:NOBS] = tiles[...].reshape(1, NOBS)

    for h in range(2):
        lanes = slice(h * HALF, (h + 1) * HALF)
        block = table[2:3, lanes] - pix * BLOCKS
        pick = jnp.where(iota((BLOCKS, HALF), 0) == block, 1.0, 0.0).astype(jnp.bfloat16)
        seen = bf16_dot(parts, pick)
        seen = seen[0:64] + seen[64:128] + seen[128:192]
        scene = iota((TIMES, HALF), 0)
        pair = jnp.where(scene == table[1:2, lanes], 1.0, 0.0) - jnp.where(
            scene == table[0:1, lanes], 1.0, 0.0
        )
        part_pred[h * OWN : (h + 1) * OWN, :] = (
            jnp.sum(seen.reshape(OWN, TIMES, HALF) * pair[None], axis=1) * (1.0 / BLK)
        )

    line_copies = [
        pltpu.make_async_remote_copy(
            part_pred, pix_pred.at[pix], pix_send.at[d], pix_recv.at[d], device_id=(mem, p), device_id_type=MESH
        )
        for d, p in enumerate(lines)
    ]
    for copy in line_copies:
        copy.start()
    for copy in line_copies:
        copy.wait()
    whole = part_pred[...]
    for p in lines:
        whole = whole + pix_pred[p]
    whole_pred[...] = whole
    mem_pred[mem] = whole

    plane_copies = [
        pltpu.make_async_remote_copy(
            whole_pred, mem_pred.at[mem], mem_send.at[d], mem_recv.at[d], device_id=(p, pix), device_id_type=MESH
        )
        for d, p in enumerate(partners)
    ]
    for copy in plane_copies:
        copy.start()
    for copy in outgoings[EARLY:]:
        copy.start()
    smalls[1].wait()
    for copy in plane_copies:
        copy.wait()

    for s in range(16):
        for h in range(2):
            predicted[OWN * s : OWN * (s + 1), h * HALF : (h + 1) * HALF] = mem_pred[s, h * OWN : (h + 1) * OWN, :]

    scale = stddev[...].reshape(1, NOBS) * math.sqrt(float(PASS_COUNT))
    pred = predicted[:, 0:NOBS]
    mean = jnp.sum(pred, axis=0, keepdims=True) * (1.0 / MEMBERS)
    scaled = (pred - mean) / (scale * ROOT)
    offset = jnp.sum(scaled * ((measured[...].reshape(1, NOBS) - mean) / scale), axis=1, keepdims=True)
    gram = f32_dot(scaled, scaled, ((1,), (1,)))
    cross = [f32_dot(scaled, noise[i], ((1,), (1,))) + offset for i in range(PASS_COUNT)]
    eye = jnp.where(iota((MEMBERS, MEMBERS), 0) == iota((MEMBERS, MEMBERS), 1), 1.0, 0.0)

    def rounded(solved):
        return (solved * (1.0 / ROOT)).astype(jnp.bfloat16).astype(jnp.float32)

    first = rounded(solve(jnp.concatenate([eye + gram, cross[0] - ROOT * gram], axis=1)))
    moved = f32_dot(gram, first)
    change = eye + first - jnp.mean(first, axis=1, keepdims=True)
    both = gram + moved
    right = jnp.concatenate([both - jnp.mean(moved, axis=1, keepdims=True), cross[1] - ROOT * both], axis=1)
    system = f32_dot(change.T, right)
    second = rounded(solve(system + jnp.concatenate([eye, jnp.zeros_like(eye)], axis=1)))
    one = first - jnp.mean(first, axis=0, keepdims=True)
    two = second - jnp.mean(second, axis=0, keepdims=True)
    total = one + two + f32_dot(one, two)
    own_share = jnp.sum(total * eye, axis=1, keepdims=True)
    factor = jnp.broadcast_to(own_share + 1.0, (MEMBERS, 128))
    total = total - own_share * eye

    widen = jnp.where(iota((MEMBERS, MEMBERS * TIMES), 1) >> 4 == iota((MEMBERS, MEMBERS * TIMES), 0), 1.0, 0.0)
    wide = bf16_dot(total.T.astype(jnp.bfloat16), widen.astype(jnp.bfloat16))
    same = (iota((TIMES, MEMBERS * TIMES), 1) & (TIMES - 1)) == iota((TIMES, MEMBERS * TIMES), 0)
    for j in range(MEMBERS):
        spread[j * TIMES : (j + 1) * TIMES, :] = jnp.where(same, wide[j : j + 1, :], 0.0).astype(jnp.bfloat16)
        keeps[j * TIMES : (j + 1) * TIMES, :] = jnp.broadcast_to(factor[j : j + 1, :], (TIMES, 128))

    mine.wait()

    def incoming(step, i):
        p = partners[i]
        return pltpu.make_async_remote_copy(
            result.at[pl.ds(OWN * p, OWN), :, columns(0, step)],
            out.at[:, :, columns(mem, step)],
            back_send.at[step, i],
            back_recv.at[step, i],
            device_id=(p, pix),
            device_id_type=MESH,
        )

    def advance(step, carry):
        for i in range(len(ORDER)):
            outgoing(step, i).wait()
        lanes = columns(0, step)
        state = received[:, :, lanes].reshape(MEMBERS * TIMES, COLS)
        for r in range(4):
            members = slice(r * 16, (r + 1) * 16)
            rows = slice(r * 256, (r + 1) * 256)
            moved = bf16_dot(spread[rows, :], state)
            kept = received[members, :, lanes].reshape(256, COLS).astype(jnp.float32)
            factors = jnp.concatenate([keeps[rows, :]] * (COLS // 128), axis=1)
            result[members, :, lanes] = (kept * factors + moved).astype(jnp.bfloat16).reshape(16, TIMES, COLS)
        for i in range(len(ORDER)):
            incoming(step, i).start()
        out[:, :, columns(mem, step)] = result[pl.ds(OWN * mem, OWN), :, lanes]
        return carry

    lax.fori_loop(0, STEPS, advance, 0)

    def finish(step, carry):
        for i in range(len(ORDER)):
            incoming(step, i).wait()
        return carry

    lax.fori_loop(0, STEPS, finish, 0)


def body(prior_motion, measured_motion, measurement_noise_stddev, gaussian_jitter, scene_couples, targeted_tile_number):
    anywhere = pl.BlockSpec(memory_space=pltpu.HBM)
    small = pl.BlockSpec(memory_space=pltpu.VMEM)
    dma = pltpu.SemaphoreType.DMA
    n = len(ORDER)
    return pl.pallas_call(
        kernel,
        out_shape=pltpu.VMEM(prior_motion.shape, jnp.bfloat16),
        in_specs=[anywhere, small, small, anywhere, anywhere, small],
        out_specs=pl.BlockSpec(memory_space=pltpu.VMEM),
        scratch_shapes=[
            pltpu.VMEM((OWN, TIMES, CELLS), jnp.bfloat16),
            pltpu.VMEM((MEMBERS, TIMES, PART), jnp.bfloat16),
            pltpu.VMEM((MEMBERS, TIMES, PART), jnp.bfloat16),
            pltpu.VMEM((MEMBERS * TIMES, MEMBERS * TIMES), jnp.bfloat16),
            pltpu.VMEM((MEMBERS * TIMES, 128), jnp.float32),
            pltpu.VMEM((PASS_COUNT, MEMBERS, NOBS), jnp.float32),
            pltpu.VMEM((2, NOBS), jnp.int32),
            pltpu.VMEM((8, OBS), jnp.int32),
            pltpu.VMEM((2 * OWN, HALF), jnp.float32),
            pltpu.VMEM((NPIX, 2 * OWN, HALF), jnp.float32),
            pltpu.VMEM((2 * OWN, HALF), jnp.float32),
            pltpu.VMEM((16, 2 * OWN, HALF), jnp.float32),
            pltpu.VMEM((MEMBERS, OBS), jnp.float32),
            dma, dma((2,)), dma,
            dma((STEPS, n)), dma((STEPS, n)),
            dma((NPIX - 1,)), dma((NPIX - 1,)),
            dma((n,)), dma((n,)),
            dma((STEPS, n)), dma((STEPS, n)),
        ],
        compiler_params=pltpu.CompilerParams(collective_id=0, has_side_effects=True, vmem_limit_bytes=59 << 20),
        name="smoother",
    )(
        prior_motion,
        measured_motion,
        measurement_noise_stddev,
        jnp.swapaxes(gaussian_jitter, 1, 2),
        scene_couples,
        targeted_tile_number,
    )


def solution(mesh):
    return jax.shard_map(
        body,
        mesh=mesh,
        in_specs=(P("mem", None, "pix"), P(), P(), P(), P(), P()),
        out_specs=P("mem", None, "pix"),
        check_vma=False,
    )
```

```python
import functools
import math

import jax
import jax.numpy as jnp
from jax import lax
from jax.experimental import pallas as pl
from jax.experimental.pallas import tpu as pltpu
from jax.sharding import PartitionSpec as P

MESH = pl.DeviceIdType.MESH
HIGHEST = lax.Precision.HIGHEST
BLK = 64
PASS_COUNT = 2
MEMBERS = 64
TIMES = 16
NOBS = 1200
CHUNK = 256
CHUNKS = -(-NOBS // CHUNK)
OWN = 4
CELLS = 32768
PART = 2048
BLOCKS = CELLS // BLK
NPIX = 8
NZ = NPIX // 2
OBS = NPIX * CHUNK
STEPS = 4
COLS = PART // STEPS
GROUP = 4
ROOT = math.sqrt(MEMBERS - 1)

ORDER = (
    (0, 1), (1, 0), (0, 3), (3, 0), (1, 1), (3, 3), (1, 3), (3, 1),
    (2, 2), (0, 2), (2, 0), (1, 2), (2, 1), (3, 2), (2, 3),
)
EARLY = 30


def iota(shape, axis):
    return lax.broadcasted_iota(jnp.int32, shape, axis)


def f32_dot(a, b, dims=((1,), (0,))):
    return lax.dot_general(a, b, (dims, ((), ())), precision=HIGHEST, preferred_element_type=jnp.float32)


def bf16_dot(a, b):
    return jnp.dot(a, b, preferred_element_type=jnp.float32)


def solve(system):
    row_at = iota(system.shape, 0)
    for start in range(0, MEMBERS, GROUP):
        columns = [jnp.broadcast_to(system[:, start + j : start + j + 1], system.shape) for j in range(GROUP)]
        for j in range(GROUP):
            k = start + j
            here = row_at == k
            inverse = 1.0 / columns[j][k : k + 1, :]
            pivot_row = system[k : k + 1, :] * inverse
            for later in range(j + 1, GROUP):
                share = columns[later][k : k + 1, :] * inverse
                columns[later] = jnp.where(here, share, columns[later] - columns[j] * share)
            system = jnp.where(here, pivot_row, system - columns[j] * pivot_row)
    return system[:, MEMBERS:]


def kernel(
    prior, measured, stddev, jitter, couples, tiles, out,
    own, received, result, spread, keeps, noise, padded_noise, levels, pairs, table,
    part_pred, pix_pred, whole_pred, mem_pred, predicted, part_sum, twin_sum, line_sum,
    load_sem, small_sem, self_sem, twin_send, twin_recv,
    send_sem, recv_sem, pix_send, pix_recv, mem_send, mem_recv, line_send, line_recv, back_send, back_recv,
):
    mem = lax.axis_index("mem")
    pix = lax.axis_index("pix")
    y = mem // 4
    x = mem % 4
    partners = [(((y + dy) % 4) * 4 + (x + dx) % 4) for dy, dx in ORDER]
    lines = [(pix + d) % NPIX for d in range(1, NPIX)]

    barrier = pltpu.get_barrier_semaphore()
    for p in partners:
        pl.semaphore_signal(barrier, 1, device_id=(p, pix), device_id_type=MESH)
    for p in lines:
        pl.semaphore_signal(barrier, 1, device_id=(mem, p), device_id_type=MESH)

    load = pltpu.make_async_copy(prior, own, load_sem)
    load.start()
    mine = pltpu.make_async_copy(
        prior.at[:, :, pl.ds(pl.multiple_of(mem * PART, PART), PART)],
        received.at[pl.ds(OWN * mem, OWN)],
        self_sem,
    )
    mine.start()
    smalls = [
        pltpu.make_async_copy(src, dst, small_sem.at[i])
        for i, (src, dst) in enumerate(
            ((couples, pairs), (jitter, noise))
        )
    ]
    for copy in smalls:
        copy.start()
    table[...] = jnp.full(table.shape, -1, jnp.int32)
    part_pred[...] = jnp.zeros(part_pred.shape, jnp.float32)
    padded_noise[:, :, 1152:] = jnp.zeros((PASS_COUNT, MEMBERS, OBS - 1152), jnp.float32)
    levels[0:1, :] = jnp.zeros((1, OBS), jnp.float32)
    levels[1:2, :] = jnp.ones((1, OBS), jnp.float32)
    levels[0:1, 0:NOBS] = measured[...].reshape(1, NOBS)
    levels[1:2, 0:NOBS] = stddev[...].reshape(1, NOBS)

    pl.semaphore_wait(barrier, len(partners) + len(lines))

    def columns(start, step):
        return pl.ds(pl.multiple_of(start * PART + step * COLS, COLS), COLS)

    def outgoing(s, i):
        p = partners[i]
        return pltpu.make_async_remote_copy(
            prior.at[:, :, columns(p, s)],
            received.at[pl.ds(OWN * mem, OWN), :, pl.ds(s * COLS, COLS)],
            send_sem.at[s, i],
            recv_sem.at[s, i],
            device_id=(p, pix),
            device_id_type=MESH,
        )

    outgoings = [outgoing(s, i) for s in range(STEPS) for i in range(len(ORDER))]
    for copy in outgoings[:EARLY]:
        copy.start()

    load.wait()
    depth = 1024

    def add_blocks(step, total):
        ones = jnp.where(iota((depth, 128), 1) - (iota((depth, 128), 0) >> 6) == step * (depth // BLK), 1.0, 0.0)
        rows = [
            own[:, :, pl.ds(pl.multiple_of(c * 8192 + step * depth, depth), depth)].reshape(OWN * TIMES, depth)
            for c in range(4)
        ]
        return total + bf16_dot(jnp.concatenate(rows, axis=0), ones.astype(jnp.bfloat16))

    sums = lax.fori_loop(0, 8192 // depth, add_blocks, jnp.zeros((4 * OWN * TIMES, 128), jnp.float32))
    sums = jnp.concatenate([sums[c * 64 : (c + 1) * 64] for c in range(4)], axis=1)
    high = sums.astype(jnp.bfloat16)
    rest = sums - high.astype(jnp.float32)
    middle = rest.astype(jnp.bfloat16)
    low = (rest - middle.astype(jnp.float32)).astype(jnp.bfloat16)
    parts = jnp.concatenate([high, middle, low], axis=0)

    smalls[0].wait()
    table[0:2, 0:NOBS] = pairs[...]
    table[2:3, 0:NOBS] = tiles[...].reshape(1, NOBS)

    for q in range(CHUNKS):
        lanes = slice(q * CHUNK, (q + 1) * CHUNK)
        pick = jnp.where(iota((BLOCKS, CHUNK), 0) == table[2:3, lanes] - pix * BLOCKS, 1.0, 0.0)
        seen = bf16_dot(parts, pick.astype(jnp.bfloat16))
        seen = seen[0:64] + seen[64:128] + seen[128:192]
        scene = iota((TIMES, CHUNK), 0)
        pair = jnp.where(scene == table[1:2, lanes], 1.0, 0.0) - jnp.where(scene == table[0:1, lanes], 1.0, 0.0)
        shift = jnp.sum(seen.reshape(OWN, TIMES, CHUNK) * pair[None], axis=1) * (1.0 / BLK)
        part_pred[q, 0:OWN, :] = shift[:, 0:128]
        part_pred[q, OWN:, :] = shift[:, 128:]

    line_copies = [
        pltpu.make_async_remote_copy(
            part_pred.at[p], pix_pred.at[pix], pix_send.at[d], pix_recv.at[d], device_id=(mem, p), device_id_type=MESH
        )
        for d, p in enumerate(lines)
    ]
    for copy in line_copies:
        copy.start()
    for copy in line_copies:
        copy.wait()
    whole = part_pred[pix]
    for p in lines:
        whole = whole + pix_pred[p]
    whole_pred[...] = whole
    mem_pred[mem] = whole

    plane_copies = [
        pltpu.make_async_remote_copy(
            whole_pred, mem_pred.at[mem], mem_send.at[d], mem_recv.at[d], device_id=(p, pix), device_id_type=MESH
        )
        for d, p in enumerate(partners)
    ]
    for copy in plane_copies:
        copy.start()
    for copy in outgoings[EARLY:]:
        copy.start()
    smalls[1].wait()
    padded_noise[:, :, 0:NOBS] = noise[...]
    for copy in plane_copies:
        copy.wait()

    for s in range(16):
        predicted[OWN * s : OWN * (s + 1), 0:128] = mem_pred[s, 0:OWN, :]
        predicted[OWN * s : OWN * (s + 1), 128:] = mem_pred[s, OWN:, :]

    chunk = pl.ds(pl.multiple_of(pix * CHUNK, CHUNK), CHUNK)
    scale = levels[1:2, chunk] * math.sqrt(float(PASS_COUNT))
    pred = predicted[...]
    mean = jnp.sum(pred, axis=0, keepdims=True) * (1.0 / MEMBERS)
    scaled = (pred - mean) / (scale * ROOT)
    offset = jnp.sum(scaled * ((levels[0:1, chunk] - mean) / scale), axis=1, keepdims=True)
    gram = f32_dot(scaled, scaled, ((1,), (1,)))
    cross = [f32_dot(scaled, padded_noise[i, :, chunk], ((1,), (1,))) + offset for i in range(PASS_COUNT)]
    part_sum[0:64, :] = jnp.concatenate([gram, cross[0]], axis=1)
    part_sum[64:96, :] = jnp.concatenate([cross[1][0:32], cross[1][32:64]], axis=1)

    core = pix % 2
    z = pix // 2
    twin = pltpu.make_async_remote_copy(
        part_sum, twin_sum, twin_send, twin_recv, device_id=(mem, z * 2 + 1 - core), device_id_type=MESH
    )
    twin.start()
    twin.wait()
    line_sum[z] = part_sum[...] + twin_sum[...]
    sum_copies = [
        pltpu.make_async_remote_copy(
            line_sum.at[z], line_sum.at[z], line_send.at[d], line_recv.at[d],
            device_id=(mem, ((z + 1 + d) % NZ) * 2 + core), device_id_type=MESH,
        )
        for d in range(NZ - 1)
    ]
    for copy in sum_copies:
        copy.start()
    for copy in sum_copies:
        copy.wait()
    products = line_sum[0] + line_sum[1] + line_sum[2] + line_sum[3]
    gram = products[0:64, 0:64]
    cross = [products[0:64, 64:128], jnp.concatenate([products[64:96, 0:64], products[64:96, 64:128]], axis=0)]
    eye = jnp.where(iota((MEMBERS, MEMBERS), 0) == iota((MEMBERS, MEMBERS), 1), 1.0, 0.0)

    def rounded(solved):
        return (solved * (1.0 / ROOT)).astype(jnp.bfloat16).astype(jnp.float32)

    first = rounded(solve(jnp.concatenate([eye + gram, cross[0] - ROOT * gram], axis=1)))
    moved = f32_dot(gram, first)
    change = eye + first - jnp.mean(first, axis=1, keepdims=True)
    both = gram + moved
    right = jnp.concatenate([both - jnp.mean(moved, axis=1, keepdims=True), cross[1] - ROOT * both], axis=1)
    system = f32_dot(change.T, right)
    second = rounded(solve(system + jnp.concatenate([eye, jnp.zeros_like(eye)], axis=1)))
    one = first - jnp.mean(first, axis=0, keepdims=True)
    two = second - jnp.mean(second, axis=0, keepdims=True)
    total = one + two + f32_dot(one, two)
    own_share = jnp.sum(total * eye, axis=1, keepdims=True)
    factor = jnp.broadcast_to(own_share + 1.0, (MEMBERS, 128))
    total = total - own_share * eye

    widen = jnp.where(iota((MEMBERS, MEMBERS * TIMES), 1) >> 4 == iota((MEMBERS, MEMBERS * TIMES), 0), 1.0, 0.0)
    wide = bf16_dot(total.T.astype(jnp.bfloat16), widen.astype(jnp.bfloat16))
    same = (iota((TIMES, MEMBERS * TIMES), 1) & (TIMES - 1)) == iota((TIMES, MEMBERS * TIMES), 0)
    for j in range(MEMBERS):
        spread[j * TIMES : (j + 1) * TIMES, :] = jnp.where(same, wide[j : j + 1, :], 0.0).astype(jnp.bfloat16)
        keeps[j * TIMES : (j + 1) * TIMES, :] = jnp.broadcast_to(factor[j : j + 1, :], (TIMES, 128))

    mine.wait()

    def incoming(step, i):
        p = partners[i]
        return pltpu.make_async_remote_copy(
            result.at[pl.ds(OWN * p, OWN), :, columns(0, step)],
            out.at[:, :, columns(mem, step)],
            back_send.at[step, i],
            back_recv.at[step, i],
            device_id=(p, pix),
            device_id_type=MESH,
        )

    def advance(step, carry):
        for i in range(len(ORDER)):
            outgoing(step, i).wait()
        lanes = columns(0, step)
        state = received[:, :, lanes].reshape(MEMBERS * TIMES, COLS)
        for r in range(4):
            members = slice(r * 16, (r + 1) * 16)
            rows = slice(r * 256, (r + 1) * 256)
            moved = bf16_dot(spread[rows, :], state)
            kept = received[members, :, lanes].reshape(256, COLS).astype(jnp.float32)
            factors = jnp.concatenate([keeps[rows, :]] * (COLS // 128), axis=1)
            result[members, :, lanes] = (kept * factors + moved).astype(jnp.bfloat16).reshape(16, TIMES, COLS)
        for i in range(len(ORDER)):
            incoming(step, i).start()
        out[:, :, columns(mem, step)] = result[pl.ds(OWN * mem, OWN), :, lanes]
        return carry

    lax.fori_loop(0, STEPS, advance, 0)

    def finish(step, carry):
        for i in range(len(ORDER)):
            incoming(step, i).wait()
        return carry

    lax.fori_loop(0, STEPS, finish, 0)


def body(prior_motion, measured_motion, measurement_noise_stddev, gaussian_jitter, scene_couples, targeted_tile_number):
    anywhere = pl.BlockSpec(memory_space=pltpu.HBM)
    small = pl.BlockSpec(memory_space=pltpu.VMEM)
    dma = pltpu.SemaphoreType.DMA
    n = len(ORDER)
    return pl.pallas_call(
        kernel,
        out_shape=pltpu.VMEM(prior_motion.shape, jnp.bfloat16),
        in_specs=[anywhere, small, small, anywhere, anywhere, small],
        out_specs=pl.BlockSpec(memory_space=pltpu.VMEM),
        scratch_shapes=[
            pltpu.VMEM((OWN, TIMES, CELLS), jnp.bfloat16),
            pltpu.VMEM((MEMBERS, TIMES, PART), jnp.bfloat16),
            pltpu.VMEM((MEMBERS, TIMES, PART), jnp.bfloat16),
            pltpu.VMEM((MEMBERS * TIMES, MEMBERS * TIMES), jnp.bfloat16),
            pltpu.VMEM((MEMBERS * TIMES, 128), jnp.float32),
            pltpu.VMEM((PASS_COUNT, MEMBERS, NOBS), jnp.float32),
            pltpu.VMEM((PASS_COUNT, MEMBERS, OBS), jnp.float32),
            pltpu.VMEM((8, OBS), jnp.float32),
            pltpu.VMEM((2, NOBS), jnp.int32),
            pltpu.VMEM((8, OBS), jnp.int32),
            pltpu.VMEM((NPIX, 2 * OWN, 128), jnp.float32),
            pltpu.VMEM((NPIX, 2 * OWN, 128), jnp.float32),
            pltpu.VMEM((2 * OWN, 128), jnp.float32),
            pltpu.VMEM((16, 2 * OWN, 128), jnp.float32),
            pltpu.VMEM((MEMBERS, CHUNK), jnp.float32),
            pltpu.VMEM((96, 128), jnp.float32),
            pltpu.VMEM((96, 128), jnp.float32),
            pltpu.VMEM((NZ, 96, 128), jnp.float32),
            dma, dma((2,)), dma, dma, dma,
            dma((STEPS, n)), dma((STEPS, n)),
            dma((NPIX - 1,)), dma((NPIX - 1,)),
            dma((n,)), dma((n,)),
            dma((NZ - 1,)), dma((NZ - 1,)),
            dma((STEPS, n)), dma((STEPS, n)),
        ],
        compiler_params=pltpu.CompilerParams(collective_id=0, has_side_effects=True, vmem_limit_bytes=59 << 20),
        name="smoother",
    )(
        prior_motion,
        measured_motion,
        measurement_noise_stddev,
        jnp.swapaxes(gaussian_jitter, 1, 2),
        scene_couples,
        targeted_tile_number,
    )


def solution(mesh):
    return jax.shard_map(
        body,
        mesh=mesh,
        in_specs=(P("mem", None, "pix"), P(), P(), P(), P(), P()),
        out_specs=P("mem", None, "pix"),
        check_vma=False,
    )
```

```python
import functools
import math

import jax
import jax.numpy as jnp
from jax import lax
from jax.experimental import pallas as pl
from jax.experimental.pallas import tpu as pltpu
from jax.sharding import PartitionSpec as P

MESH = pl.DeviceIdType.MESH
HIGHEST = lax.Precision.HIGHEST
BLK = 64
PASS_COUNT = 2
MEMBERS = 64
TIMES = 16
NOBS = 1200
CHUNK = 256
CHUNKS = -(-NOBS // CHUNK)
OWN = 4
CELLS = 32768
PART = 2048
BLOCKS = CELLS // BLK
NPIX = 8
NZ = NPIX // 2
OBS = NPIX * CHUNK
STEPS = 4
COLS = PART // STEPS
GROUP = 4
ROOT = math.sqrt(MEMBERS - 1)

ORDER = (
    (0, 1), (1, 0), (0, 3), (3, 0), (1, 1), (3, 3), (1, 3), (3, 1),
    (2, 2), (0, 2), (2, 0), (1, 2), (2, 1), (3, 2), (2, 3),
)
EARLY = 30


def iota(shape, axis):
    return lax.broadcasted_iota(jnp.int32, shape, axis)


def f32_dot(a, b, dims=((1,), (0,))):
    return lax.dot_general(a, b, (dims, ((), ())), precision=HIGHEST, preferred_element_type=jnp.float32)


def bf16_dot(a, b):
    return jnp.dot(a, b, preferred_element_type=jnp.float32)


def solve(system):
    row_at = iota(system.shape, 0)
    for start in range(0, MEMBERS, GROUP):
        columns = [jnp.broadcast_to(system[:, start + j : start + j + 1], system.shape) for j in range(GROUP)]
        for j in range(GROUP):
            k = start + j
            here = row_at == k
            inverse = 1.0 / columns[j][k : k + 1, :]
            pivot_row = system[k : k + 1, :] * inverse
            for later in range(j + 1, GROUP):
                share = columns[later][k : k + 1, :] * inverse
                columns[later] = jnp.where(here, share, columns[later] - columns[j] * share)
            system = jnp.where(here, pivot_row, system - columns[j] * pivot_row)
    return system[:, MEMBERS:]


def kernel(
    prior, measured, stddev, jitter, couples, tiles, out,
    own, received, result, spread, keeps, noise, padded_noise, levels, pairs, table,
    part_pred, pix_pred, whole_pred, mem_pred, predicted, part_sum, twin_sum, line_sum,
    load_sem, small_sem, self_sem, twin_send, twin_recv,
    send_sem, recv_sem, pix_send, pix_recv, mem_send, mem_recv, line_send, line_recv, back_send, back_recv,
):
    mem = lax.axis_index("mem")
    pix = lax.axis_index("pix")
    y = mem // 4
    x = mem % 4
    side = pix % 2
    partners = [
        ((y + dy + side * (dx - dy) + 4) % 4) * 4 + (x + dx + side * (dy - dx) + 4) % 4 for dy, dx in ORDER
    ]
    lines = [(pix + d) % NPIX for d in range(1, NPIX)]

    barrier = pltpu.get_barrier_semaphore()
    for p in partners:
        pl.semaphore_signal(barrier, 1, device_id=(p, pix), device_id_type=MESH)
    for p in lines:
        pl.semaphore_signal(barrier, 1, device_id=(mem, p), device_id_type=MESH)

    load = pltpu.make_async_copy(prior, own, load_sem)
    load.start()
    mine = pltpu.make_async_copy(
        prior.at[:, :, pl.ds(pl.multiple_of(mem * PART, PART), PART)],
        received.at[pl.ds(OWN * mem, OWN)],
        self_sem,
    )
    mine.start()
    smalls = [
        pltpu.make_async_copy(src, dst, small_sem.at[i])
        for i, (src, dst) in enumerate(
            ((couples, pairs), (jitter, noise))
        )
    ]
    for copy in smalls:
        copy.start()
    table[...] = jnp.full(table.shape, -1, jnp.int32)
    part_pred[...] = jnp.zeros(part_pred.shape, jnp.float32)
    padded_noise[:, :, 1152:] = jnp.zeros((PASS_COUNT, MEMBERS, OBS - 1152), jnp.float32)
    levels[0:1, :] = jnp.zeros((1, OBS), jnp.float32)
    levels[1:2, :] = jnp.ones((1, OBS), jnp.float32)
    levels[0:1, 0:NOBS] = measured[...].reshape(1, NOBS)
    levels[1:2, 0:NOBS] = stddev[...].reshape(1, NOBS)

    pl.semaphore_wait(barrier, len(partners) + len(lines))

    def columns(start, step):
        return pl.ds(pl.multiple_of(start * PART + step * COLS, COLS), COLS)

    def outgoing(s, i):
        p = partners[i]
        return pltpu.make_async_remote_copy(
            prior.at[:, :, columns(p, s)],
            received.at[pl.ds(OWN * mem, OWN), :, pl.ds(s * COLS, COLS)],
            send_sem.at[s, i],
            recv_sem.at[s, i],
            device_id=(p, pix),
            device_id_type=MESH,
        )

    outgoings = [outgoing(s, i) for s in range(STEPS) for i in range(len(ORDER))]
    for copy in outgoings[:EARLY]:
        copy.start()

    load.wait()
    depth = 1024

    def add_blocks(step, total):
        ones = jnp.where(iota((depth, 128), 1) - (iota((depth, 128), 0) >> 6) == step * (depth // BLK), 1.0, 0.0)
        rows = [
            own[:, :, pl.ds(pl.multiple_of(c * 8192 + step * depth, depth), depth)].reshape(OWN * TIMES, depth)
            for c in range(4)
        ]
        return total + bf16_dot(jnp.concatenate(rows, axis=0), ones.astype(jnp.bfloat16))

    sums = lax.fori_loop(0, 8192 // depth, add_blocks, jnp.zeros((4 * OWN * TIMES, 128), jnp.float32))
    sums = jnp.concatenate([sums[c * 64 : (c + 1) * 64] for c in range(4)], axis=1)
    high = sums.astype(jnp.bfloat16)
    rest = sums - high.astype(jnp.float32)
    middle = rest.astype(jnp.bfloat16)
    low = (rest - middle.astype(jnp.float32)).astype(jnp.bfloat16)
    parts = jnp.concatenate([high, middle, low], axis=0)

    smalls[0].wait()
    table[0:2, 0:NOBS] = pairs[...]
    table[2:3, 0:NOBS] = tiles[...].reshape(1, NOBS)

    for q in range(CHUNKS):
        lanes = slice(q * CHUNK, (q + 1) * CHUNK)
        pick = jnp.where(iota((BLOCKS, CHUNK), 0) == table[2:3, lanes] - pix * BLOCKS, 1.0, 0.0)
        seen = bf16_dot(parts, pick.astype(jnp.bfloat16))
        seen = seen[0:64] + seen[64:128] + seen[128:192]
        scene = iota((TIMES, CHUNK), 0)
        pair = jnp.where(scene == table[1:2, lanes], 1.0, 0.0) - jnp.where(scene == table[0:1, lanes], 1.0, 0.0)
        shift = jnp.sum(seen.reshape(OWN, TIMES, CHUNK) * pair[None], axis=1) * (1.0 / BLK)
        part_pred[q, 0:OWN, :] = shift[:, 0:128]
        part_pred[q, OWN:, :] = shift[:, 128:]

    line_copies = [
        pltpu.make_async_remote_copy(
            part_pred.at[p], pix_pred.at[pix], pix_send.at[d], pix_recv.at[d], device_id=(mem, p), device_id_type=MESH
        )
        for d, p in enumerate(lines)
    ]
    for copy in line_copies:
        copy.start()
    for copy in line_copies:
        copy.wait()
    whole = part_pred[pix]
    for p in lines:
        whole = whole + pix_pred[p]
    whole_pred[...] = whole
    mem_pred[mem] = whole

    plane_copies = [
        pltpu.make_async_remote_copy(
            whole_pred, mem_pred.at[mem], mem_send.at[d], mem_recv.at[d], device_id=(p, pix), device_id_type=MESH
        )
        for d, p in enumerate(partners)
    ]
    for copy in plane_copies:
        copy.start()
    for copy in outgoings[EARLY:]:
        copy.start()
    smalls[1].wait()
    padded_noise[:, :, 0:NOBS] = noise[...]
    for copy in plane_copies:
        copy.wait()

    for s in range(16):
        predicted[OWN * s : OWN * (s + 1), 0:128] = mem_pred[s, 0:OWN, :]
        predicted[OWN * s : OWN * (s + 1), 128:] = mem_pred[s, OWN:, :]

    chunk = pl.ds(pl.multiple_of(pix * CHUNK, CHUNK), CHUNK)
    scale = levels[1:2, chunk] * math.sqrt(float(PASS_COUNT))
    pred = predicted[...]
    mean = jnp.sum(pred, axis=0, keepdims=True) * (1.0 / MEMBERS)
    scaled = (pred - mean) / (scale * ROOT)
    offset = jnp.sum(scaled * ((levels[0:1, chunk] - mean) / scale), axis=1, keepdims=True)
    gram = f32_dot(scaled, scaled, ((1,), (1,)))
    cross = [f32_dot(scaled, padded_noise[i, :, chunk], ((1,), (1,))) + offset for i in range(PASS_COUNT)]
    part_sum[0:64, :] = jnp.concatenate([gram, cross[0]], axis=1)
    part_sum[64:96, :] = jnp.concatenate([cross[1][0:32], cross[1][32:64]], axis=1)

    core = pix % 2
    z = pix // 2
    twin = pltpu.make_async_remote_copy(
        part_sum, twin_sum, twin_send, twin_recv, device_id=(mem, z * 2 + 1 - core), device_id_type=MESH
    )
    twin.start()
    twin.wait()
    line_sum[z] = part_sum[...] + twin_sum[...]
    sum_copies = [
        pltpu.make_async_remote_copy(
            line_sum.at[z], line_sum.at[z], line_send.at[d], line_recv.at[d],
            device_id=(mem, ((z + 1 + d) % NZ) * 2 + core), device_id_type=MESH,
        )
        for d in range(NZ - 1)
    ]
    for copy in sum_copies:
        copy.start()
    for copy in sum_copies:
        copy.wait()
    products = line_sum[0] + line_sum[1] + line_sum[2] + line_sum[3]
    gram = products[0:64, 0:64]
    cross = [products[0:64, 64:128], jnp.concatenate([products[64:96, 0:64], products[64:96, 64:128]], axis=0)]
    eye = jnp.where(iota((MEMBERS, MEMBERS), 0) == iota((MEMBERS, MEMBERS), 1), 1.0, 0.0)

    def rounded(solved):
        return (solved * (1.0 / ROOT)).astype(jnp.bfloat16).astype(jnp.float32)

    first = rounded(solve(jnp.concatenate([eye + gram, cross[0] - ROOT * gram], axis=1)))
    moved = f32_dot(gram, first)
    change = eye + first - jnp.mean(first, axis=1, keepdims=True)
    both = gram + moved
    right = jnp.concatenate([both - jnp.mean(moved, axis=1, keepdims=True), cross[1] - ROOT * both], axis=1)
    system = f32_dot(change.T, right)
    second = rounded(solve(system + jnp.concatenate([eye, jnp.zeros_like(eye)], axis=1)))
    one = first - jnp.mean(first, axis=0, keepdims=True)
    two = second - jnp.mean(second, axis=0, keepdims=True)
    total = one + two + f32_dot(one, two)
    own_share = jnp.sum(total * eye, axis=1, keepdims=True)
    factor = jnp.broadcast_to(own_share + 1.0, (MEMBERS, 128))
    total = total - own_share * eye

    widen = jnp.where(iota((MEMBERS, MEMBERS * TIMES), 1) >> 4 == iota((MEMBERS, MEMBERS * TIMES), 0), 1.0, 0.0)
    wide = bf16_dot(total.T.astype(jnp.bfloat16), widen.astype(jnp.bfloat16))
    same = (iota((TIMES, MEMBERS * TIMES), 1) & (TIMES - 1)) == iota((TIMES, MEMBERS * TIMES), 0)
    for j in range(MEMBERS):
        spread[j * TIMES : (j + 1) * TIMES, :] = jnp.where(same, wide[j : j + 1, :], 0.0).astype(jnp.bfloat16)
        keeps[j * TIMES : (j + 1) * TIMES, :] = jnp.broadcast_to(factor[j : j + 1, :], (TIMES, 128))

    mine.wait()

    def incoming(step, i):
        p = partners[i]
        return pltpu.make_async_remote_copy(
            result.at[pl.ds(OWN * p, OWN), :, columns(0, step)],
            out.at[:, :, columns(mem, step)],
            back_send.at[step, i],
            back_recv.at[step, i],
            device_id=(p, pix),
            device_id_type=MESH,
        )

    def advance(step, carry):
        for i in range(len(ORDER)):
            outgoing(step, i).wait()
        lanes = columns(0, step)
        state = received[:, :, lanes].reshape(MEMBERS * TIMES, COLS)
        for r in range(4):
            members = slice(r * 16, (r + 1) * 16)
            rows = slice(r * 256, (r + 1) * 256)
            moved = bf16_dot(spread[rows, :], state)
            kept = received[members, :, lanes].reshape(256, COLS).astype(jnp.float32)
            factors = jnp.concatenate([keeps[rows, :]] * (COLS // 128), axis=1)
            result[members, :, lanes] = (kept * factors + moved).astype(jnp.bfloat16).reshape(16, TIMES, COLS)
        for i in range(len(ORDER)):
            incoming(step, i).start()
        out[:, :, columns(mem, step)] = result[pl.ds(OWN * mem, OWN), :, lanes]
        return carry

    lax.fori_loop(0, STEPS, advance, 0)

    def finish(step, carry):
        for i in range(len(ORDER)):
            incoming(step, i).wait()
        return carry

    lax.fori_loop(0, STEPS, finish, 0)


def body(prior_motion, measured_motion, measurement_noise_stddev, gaussian_jitter, scene_couples, targeted_tile_number):
    anywhere = pl.BlockSpec(memory_space=pltpu.HBM)
    small = pl.BlockSpec(memory_space=pltpu.VMEM)
    dma = pltpu.SemaphoreType.DMA
    n = len(ORDER)
    return pl.pallas_call(
        kernel,
        out_shape=pltpu.VMEM(prior_motion.shape, jnp.bfloat16),
        in_specs=[anywhere, small, small, anywhere, anywhere, small],
        out_specs=pl.BlockSpec(memory_space=pltpu.VMEM),
        scratch_shapes=[
            pltpu.VMEM((OWN, TIMES, CELLS), jnp.bfloat16),
            pltpu.VMEM((MEMBERS, TIMES, PART), jnp.bfloat16),
            pltpu.VMEM((MEMBERS, TIMES, PART), jnp.bfloat16),
            pltpu.VMEM((MEMBERS * TIMES, MEMBERS * TIMES), jnp.bfloat16),
            pltpu.VMEM((MEMBERS * TIMES, 128), jnp.float32),
            pltpu.VMEM((PASS_COUNT, MEMBERS, NOBS), jnp.float32),
            pltpu.VMEM((PASS_COUNT, MEMBERS, OBS), jnp.float32),
            pltpu.VMEM((8, OBS), jnp.float32),
            pltpu.VMEM((2, NOBS), jnp.int32),
            pltpu.VMEM((8, OBS), jnp.int32),
            pltpu.VMEM((NPIX, 2 * OWN, 128), jnp.float32),
            pltpu.VMEM((NPIX, 2 * OWN, 128), jnp.float32),
            pltpu.VMEM((2 * OWN, 128), jnp.float32),
            pltpu.VMEM((16, 2 * OWN, 128), jnp.float32),
            pltpu.VMEM((MEMBERS, CHUNK), jnp.float32),
            pltpu.VMEM((96, 128), jnp.float32),
            pltpu.VMEM((96, 128), jnp.float32),
            pltpu.VMEM((NZ, 96, 128), jnp.float32),
            dma, dma((2,)), dma, dma, dma,
            dma((STEPS, n)), dma((STEPS, n)),
            dma((NPIX - 1,)), dma((NPIX - 1,)),
            dma((n,)), dma((n,)),
            dma((NZ - 1,)), dma((NZ - 1,)),
            dma((STEPS, n)), dma((STEPS, n)),
        ],
        compiler_params=pltpu.CompilerParams(collective_id=0, has_side_effects=True, vmem_limit_bytes=59 << 20),
        name="smoother",
    )(
        prior_motion,
        measured_motion,
        measurement_noise_stddev,
        jnp.swapaxes(gaussian_jitter, 1, 2),
        scene_couples,
        targeted_tile_number,
    )


def solution(mesh):
    return jax.shard_map(
        body,
        mesh=mesh,
        in_specs=(P("mem", None, "pix"), P(), P(), P(), P(), P()),
        out_specs=P("mem", None, "pix"),
        check_vma=False,
    )
```
